128 devices in a mesh: rep: 1, r: 4 (over x), s: 32 (over y, z, core).
Axes of the slice: x: 4, y: 4, z: 4, core: 2. Of those that a mesh axis runs over, the one named last changes fastest.
Arguments:
- x: bfloat16 [128, 2048, 1280], P(('rep', 'r', 's'))
- dy: bfloat16 [128, 2048, 1280], P(('rep', 'r', 's'))
- w_gate: bfloat16 [2, 1280, 4352], P(None, 's')
- w_up: bfloat16 [2, 1280, 4352], P(None, 's')
- w_down: bfloat16 [2, 4352, 1280], P(None, 's')
Outputs:
- output 1: bfloat16 [128, 2048, 1280], P(('rep', 'r', 's'))
- output 2: bfloat16 [2, 1280, 4352], P('rep', 's')
- output 3: bfloat16 [2, 1280, 4352], P('rep', 's')
- output 4: bfloat16 [2, 4352, 1280], P('rep', 's')
All inputs are finite; a program needn't handle non-finite values.
Results may differ from the reference program's by a relative error of at most 0.018.
Values are sent between devices in bfloat16 or wider.
A program may use at most 1.5 GiB of HBM per device.

```python
import jax
import jax.numpy as jnp
from jax import lax

SEQUENCES = 128
TOKENS = 2048
D = 1280
FF = 4352
LAYERS = 2
NAMES = ("w_gate", "w_up", "w_down")
SHAPES = {"w_gate": (LAYERS, D, FF), "w_up": (LAYERS, D, FF), "w_down": (LAYERS, FF, D)}


def bump(key, n, height):
    away = (jnp.arange(n, dtype=jnp.int32) - jax.random.randint(key, (), 0, n, jnp.int32)) % n
    return jnp.where(away < n // 8, height, 1.0)


def together(key, own, strength):
    shared = jax.random.normal(key, own.shape[1:], jnp.float32)
    return (own + strength * shared) * lax.rsqrt(1 + strength * strength)


def setup_inputs(seed: int = 0, part: int = 0) -> dict:
    kx, kdy, ka, kb, kz, kf, kh, kl, *kw = jax.random.split(jax.random.key(seed), 8 + len(NAMES))
    kx, kdy, ka, kb = (jax.random.fold_in(k, part) for k in (kx, kdy, ka, kb))
    shape = (SEQUENCES, TOKENS, D)
    much_x, much_dy = jax.random.uniform(kz, (2,), jnp.float32, 0.0, 1.0)
    layers = 2.0 ** jax.random.uniform(kl, (LAYERS, 1, 1), jnp.float32, -1.0, 1.0)
    x = together(ka, jax.random.normal(kx, shape, jnp.float32), much_x) * bump(kf, D, 4.0)
    dy = together(kb, jax.random.normal(kdy, shape, jnp.float32), much_dy)
    drawn = {"x": x.astype(jnp.bfloat16), "dy": (dy * (SEQUENCES * TOKENS) ** -0.5).astype(jnp.bfloat16)}
    for key, name in zip(kw, NAMES, strict=True):
        w = jax.random.normal(key, SHAPES[name], jnp.float32) * SHAPES[name][1] ** -0.5
        drawn[name] = (w * {"w_gate": 1.0, "w_up": bump(kh, FF, 4.0), "w_down": layers}[name]).astype(jnp.bfloat16)
    return drawn


def matmul(a, w):
    return jnp.dot(a, w, preferred_element_type=jnp.float32).astype(jnp.bfloat16)


def normed(h):
    wide = h.astype(jnp.float32)
    scale = lax.rsqrt(jnp.mean(wide**2, -1, keepdims=True) + 1e-6)
    return (wide * scale).astype(jnp.bfloat16)


def layer(h, w):
    a = normed(h)
    gate = jnp.dot(a, w["w_gate"], preferred_element_type=jnp.float32)
    up = jnp.dot(a, w["w_up"], preferred_element_type=jnp.float32)
    return h + matmul((jax.nn.silu(gate) * up).astype(jnp.bfloat16), w["w_down"])


def stack(weights, h):
    return lax.scan(lambda h, w: (layer(h, w), None), h, weights)[0]


def reference(x, dy, w_gate, w_up, w_down):
    weights = dict(zip(NAMES, (w_gate, w_up, w_down), strict=True))

    def take(so_far, sequence):
        h, by_y = sequence
        _, back = jax.vjp(stack, weights, h)
        by_weights, by_h = back(by_y)
        return jax.tree.map(lambda total, term: total + term.astype(jnp.float32), so_far, by_weights), by_h

    none_yet = {name: jnp.zeros(w.shape, jnp.float32) for name, w in weights.items()}
    by_weights, by_x = lax.scan(take, none_yet, (x, dy))
    return (by_x, *(by_weights[name].astype(jnp.bfloat16) for name in NAMES))
```

```python
import functools

import jax
import jax.numpy as jnp
from jax import lax
from jax.experimental import pallas as pl
from jax.experimental.pallas import tpu as pltpu
from jax.sharding import PartitionSpec as P

F32, BF16 = jnp.float32, jnp.bfloat16
SIDE = 4
VMEM_BYTES = 66 * 2**20 - 2**18


def matmul(a, w):
    return jnp.dot(a, w, preferred_element_type=F32).astype(BF16)


def dot_f32(a, w):
    return jnp.dot(a, w, preferred_element_type=F32)


def dot_nt(a, w):
    return lax.dot_general(a, w, (((1,), (1,)), ((), ())), preferred_element_type=F32).astype(BF16)


def dot_tn(a, w):
    return lax.dot_general(a, w, (((0,), (0,)), ((), ())), preferred_element_type=F32).astype(BF16)


def normed(h):
    wide = h.astype(F32)
    scale = lax.rsqrt(jnp.mean(wide**2, -1, keepdims=True) + 1e-6)
    return (wide * scale).astype(BF16)


def act(gate, up):
    return (jax.nn.silu(gate) * up).astype(BF16)


class Place:
    def __init__(self):
        self.s = lax.axis_index("s")
        self.r = lax.axis_index("r")
        self.k = self.s % 2
        self.y = self.s // (2 * SIDE)
        self.z = (self.s // 2) % SIDE
        self.b = self.y + self.k * (self.z - self.y)
        self.a = self.z + self.k * (self.y - self.z)

    def at(self, b, a):
        b, a = b % SIDE, a % SIDE
        y = b + self.k * (a - b)
        z = a + self.k * (b - a)
        return {"s": (y * SIDE + z) * 2 + self.k}

    def partner(self):
        return {"s": self.s + 1 - 2 * self.k}

    def group(self, bit):
        if bit == 1:
            return {"r": self.r + 1 - 2 * (self.r % 2)}
        return {"r": (self.r + 2) % 4}


MESH = pl.DeviceIdType.MESH


def send(src, dst, send_sem, recv_sem, to):
    return pltpu.make_async_remote_copy(src_ref=src, dst_ref=dst, send_sem=send_sem, recv_sem=recv_sem, device_id=to, device_id_type=MESH)


def meet(devices):
    barrier = pltpu.get_barrier_semaphore()
    for to in devices:
        pl.semaphore_signal(barrier, inc=1, device_id=to, device_id_type=MESH)
    pl.semaphore_wait(barrier, len(devices))


def wide(ref):
    return ref.astype(F32)


class Sum:
    def __init__(self, at, way, term, out, mine, theirs, rec, arec, xs, xr, sems):
        self.at, self.way, self.term, self.out = at, way, term, out
        self.mine, self.theirs, self.rec, self.arec, self.xs, self.xr = mine, theirs, rec, arec, xs, xr
        (self.local, self.pair_s, self.pair_r, self.b_s, self.b_r, self.a_s, self.a_r, self.x_s, self.x_r) = sems
        self.started = []

    def remote(self, *args):
        copy = send(*args)
        copy.start()
        self.started.append(copy)
        return copy

    def start(self):
        at = self.at
        self.loads = []
        self.pairs = []
        for j in range(SIDE):
            for core, (own, away) in enumerate(((self.term.at[j, :, 0], self.term.at[:, j, 1]), (self.term.at[:, j, 1], self.term.at[j, :, 0]))):
                load = pltpu.make_async_copy(own, self.mine.at[j], self.local.at[j])
                pair = send(away, self.theirs.at[j], self.pair_s.at[j], self.pair_r.at[j], at.partner())

                @pl.when(at.k == core)
                def _(load=load, pair=pair):
                    pair.start()
                    load.start()

                if core == 0:
                    self.loads.append(load)
                    self.pairs.append(pair)
        self.started += self.pairs

    def block(self, b, extra=()):
        @pl.loop(0, SIDE)
        def _(j):
            total = wide(self.mine[b, j]) + wide(self.theirs[b, j])
            for slot in extra:
                total = total + wide(self.rec[slot, j])
            self.theirs[b, j] = total.astype(BF16)

    def line(self, a):
        b = self.at.b
        return wide(self.mine[b, a]) + wide(self.theirs[b, a]) + wide(self.rec[1, a]) + wide(self.rec[2, a])

    def first(self):
        for load in self.loads:
            load.wait()
        for pair in self.pairs:
            pair.wait_recv()
        at, w = self.at, self.way
        far, back = (at.b + 2) % SIDE, (at.b - w) % SIDE
        self.block(far)
        self.far = self.remote(self.theirs.at[far], self.rec.at[0], self.b_s.at[0], self.b_r.at[0], at.at(at.b + w, at.a))
        self.block(back)
        self.back = self.remote(self.theirs.at[back], self.rec.at[2], self.b_s.at[2], self.b_r.at[2], at.at(at.b - w, at.a))

    def second(self):
        at, w = self.at, self.way
        near = (at.b + w) % SIDE
        self.far.wait_recv()
        self.block(near, (0,))
        self.near = self.remote(self.theirs.at[near], self.rec.at[1], self.b_s.at[1], self.b_r.at[1], at.at(at.b + w, at.a))

    def third(self):
        at, w = self.at, self.way
        self.back.wait_recv()
        self.near.wait_recv()
        far, back = (at.a + 2) % SIDE, (at.a - w) % SIDE
        self.theirs[at.b, far] = self.line(far).astype(BF16)
        self.far = self.remote(self.theirs.at[at.b, far], self.arec.at[0], self.a_s.at[0], self.a_r.at[0], at.at(at.b, at.a + w))
        self.theirs[at.b, back] = self.line(back).astype(BF16)
        self.back = self.remote(self.theirs.at[at.b, back], self.arec.at[2], self.a_s.at[2], self.a_r.at[2], at.at(at.b, at.a - w))

    def fourth(self):
        at, w = self.at, self.way
        near = (at.a + w) % SIDE
        self.far.wait_recv()
        self.theirs[at.b, near] = (self.line(near) + wide(self.arec[0])).astype(BF16)
        self.near = self.remote(self.theirs.at[at.b, near], self.arec.at[1], self.a_s.at[1], self.a_r.at[1], at.at(at.b, at.a + w))

    def fifth(self):
        at = self.at
        self.back.wait_recv()
        self.near.wait_recv()
        self.xs[0] = (self.line(at.a) + wide(self.arec[1]) + wide(self.arec[2])).astype(BF16)
        self.cross = self.remote(self.xs.at[0], self.xr.at[0], self.x_s.at[0], self.x_r.at[0], at.group(1))

    def sixth(self):
        self.cross.wait_recv()
        self.xs[1] = (wide(self.xs[0]) + wide(self.xr[0])).astype(BF16)
        self.cross = self.remote(self.xs.at[1], self.xr.at[1], self.x_s.at[1], self.x_r.at[1], self.at.group(2))

    def last(self):
        self.cross.wait_recv()
        self.out[...] = (wide(self.xs[1]) + wide(self.xr[1])).astype(BF16)

    def end(self):
        for copy in self.started:
            copy.wait_send()

    STAGES = ("start", "first", "second", "third", "fourth", "fifth", "sixth", "last", "end")


def sum_scratch(rows, columns):
    block, dma = (rows, columns), pltpu.SemaphoreType.DMA
    bufs = [pltpu.VMEM((SIDE, SIDE) + block, BF16)] * 2 + [pltpu.VMEM((3, SIDE) + block, BF16), pltpu.VMEM((3,) + block, BF16)]
    bufs += [pltpu.VMEM((2,) + block, BF16)] * 2
    return bufs + [dma((4,))] * 3 + [dma((3,))] * 4 + [dma((2,))] * 2


def summed(*terms, collective_id=1):
    shaped = [t.reshape(SIDE, SIDE, 2, t.shape[0] // 32, t.shape[1]) for t in terms]
    blocks = [t.shape[3:] for t in shaped]
    n = len(terms)

    def kernel(*refs):
        at = Place()
        ins, outs, scratch = refs[:n], refs[n : 2 * n], refs[2 * n :]
        sums = []
        for i in range(n):
            mine, theirs, rec, arec, xs, xr, *sems = scratch[15 * i : 15 * i + 15]
            sums.append(Sum(at, 1 if i % 2 == 0 else -1, ins[i], outs[i], mine, theirs, rec, arec, xs, xr, sems))
        meet([at.at(at.b + 1, at.a), at.at(at.b - 1, at.a), at.at(at.b, at.a + 1), at.at(at.b, at.a - 1), at.partner(), at.group(1), at.group(2)])
        for stage in Sum.STAGES:
            for one in sums:
                getattr(one, stage)()

    return pl.pallas_call(
        kernel,
        out_shape=[jax.ShapeDtypeStruct(block, BF16) for block in blocks],
        in_specs=[pl.BlockSpec(memory_space=pl.ANY)] * n,
        out_specs=[pl.BlockSpec(memory_space=pltpu.VMEM)] * n,
        scratch_shapes=[one for block in blocks for one in sum_scratch(*block)],
        compiler_params=pltpu.CompilerParams(collective_id=collective_id, has_side_effects=True, vmem_limit_bytes=VMEM_BYTES),
        name="summed",
    )(*shaped)


def solution(mesh):
    def fetched(w):
        return lax.all_gather(w, "s", axis=0, tiled=True)

    def scattered(term):
        return lax.psum(lax.psum_scatter(term, "s", scatter_dimension=0, tiled=True), "r")

    def step(x, dy, w_gate, w_up, w_down):
        x, dy = x[0], dy[0]
        gate0, up0, down0 = fetched(w_gate[0]), fetched(w_up[0]), fetched(w_down[0])
        gate1, up1, down1 = fetched(w_gate[1]), fetched(w_up[1]), fetched(w_down[1])

        a0, back_norm0 = jax.vjp(normed, x)
        g0, u0 = dot_f32(a0, gate0), dot_f32(a0, up0)
        m0, back_act0 = jax.vjp(act, g0, u0)
        h1 = x + matmul(m0, down0)
        a1, back_norm1 = jax.vjp(normed, h1)
        g1, u1 = dot_f32(a1, gate1), dot_f32(a1, up1)
        m1, back_act1 = jax.vjp(act, g1, u1)

        by_down1 = scattered(dot_tn(m1, dy))
        dg1, du1 = back_act1(dot_nt(dy, down1))
        dg1, du1 = dg1.astype(BF16), du1.astype(BF16)
        by_gate1 = scattered(dot_tn(a1, dg1))
        by_up1 = scattered(dot_tn(a1, du1))
        by_h1 = dy + back_norm1(dot_nt(dg1, gate1) + dot_nt(du1, up1))[0]

        t_down0 = dot_tn(m0, by_h1)
        dg0, du0 = back_act0(dot_nt(by_h1, down0))
        dg0, du0 = dg0.astype(BF16), du0.astype(BF16)
        t_gate0, t_up0 = dot_tn(a0, dg0), dot_tn(a0, du0)
        by_x = by_h1 + back_norm0(dot_nt(dg0, gate0) + dot_nt(du0, up0))[0]
        by_down0, by_gate0, by_up0 = summed(t_down0, t_gate0, t_up0)
        return by_x[None], jnp.stack([by_gate0, by_gate1]), jnp.stack([by_up0, by_up1]), jnp.stack([by_down0, by_down1])

    states, cut = P(("rep", "r", "s"), None, None), P(None, "s", None)
    return jax.shard_map(
        step,
        mesh=mesh,
        in_specs=(states, states) + (cut,) * 3,
        out_specs=(states,) + (P("rep", "s", None),) * 3,
        check_vma=False,
    )
```

```python
import functools

import jax
import jax.numpy as jnp
from jax import lax
from jax.experimental import pallas as pl
from jax.experimental.pallas import tpu as pltpu
from jax.sharding import PartitionSpec as P

F32, BF16 = jnp.float32, jnp.bfloat16
SIDE = 4
VMEM_BYTES = 66 * 2**20 - 2**18


def matmul(a, w):
    return jnp.dot(a, w, preferred_element_type=F32).astype(BF16)


def dot_f32(a, w):
    return jnp.dot(a, w, preferred_element_type=F32)


def dot_nt(a, w):
    return lax.dot_general(a, w, (((1,), (1,)), ((), ())), preferred_element_type=F32).astype(BF16)


def dot_tn(a, w):
    return lax.dot_general(a, w, (((0,), (0,)), ((), ())), preferred_element_type=F32).astype(BF16)


def normed(h):
    wide = h.astype(F32)
    scale = lax.rsqrt(jnp.mean(wide**2, -1, keepdims=True) + 1e-6)
    return (wide * scale).astype(BF16)


def act(gate, up):
    return (jax.nn.silu(gate) * up).astype(BF16)


class Place:
    def __init__(self):
        self.s = lax.axis_index("s")
        self.r = lax.axis_index("r")
        self.k = self.s % 2
        self.y = self.s // (2 * SIDE)
        self.z = (self.s // 2) % SIDE
        self.b = self.y + self.k * (self.z - self.y)
        self.a = self.z + self.k * (self.y - self.z)

    def at(self, b, a):
        b, a = b % SIDE, a % SIDE
        y = b + self.k * (a - b)
        z = a + self.k * (b - a)
        return {"s": (y * SIDE + z) * 2 + self.k}

    def partner(self):
        return {"s": self.s + 1 - 2 * self.k}

    def group(self, bit):
        if bit == 1:
            return {"r": self.r + 1 - 2 * (self.r % 2)}
        return {"r": (self.r + 2) % 4}


MESH = pl.DeviceIdType.MESH


def send(src, dst, send_sem, recv_sem, to):
    return pltpu.make_async_remote_copy(src_ref=src, dst_ref=dst, send_sem=send_sem, recv_sem=recv_sem, device_id=to, device_id_type=MESH)


def meet(devices):
    barrier = pltpu.get_barrier_semaphore()
    for to in devices:
        pl.semaphore_signal(barrier, inc=1, device_id=to, device_id_type=MESH)
    pl.semaphore_wait(barrier, len(devices))


def wide(ref):
    return ref.astype(F32)


class Sum:
    STAGES = ("start", "first", "second", "third", "fourth", "fifth", "sixth", "last", "end")

    def __init__(self, at, way, term, out, mine, theirs, rec, arec, xs, xr, local, pair_s, pair_r, b_s, b_r, a_s, a_r, x_s, x_r):
        self.at, self.out = at, out
        self.mine, self.theirs, self.rec, self.arec, self.xs, self.xr = mine, theirs, rec, arec, xs, xr
        b, a = at.b, at.a
        self.b_far, self.b_near, self.b_back = (b + 2) % SIDE, (b + way) % SIDE, (b - way) % SIDE
        self.a_far, self.a_near, self.a_back = (a + 2) % SIDE, (a + way) % SIDE, (a - way) % SIDE
        self.loads, self.pairs = [[], []], [[], []]
        for j in range(SIDE):
            for core, (own, away) in enumerate(((term.at[j, :, 0], term.at[:, j, 1]), (term.at[:, j, 1], term.at[j, :, 0]))):
                self.loads[core].append(pltpu.make_async_copy(own, mine.at[j], local.at[j]))
                self.pairs[core].append(send(away, theirs.at[j], pair_s.at[j], pair_r.at[j], at.partner()))
        ahead, behind = at.at(b + way, a), at.at(b - way, a)
        self.far = send(theirs.at[self.b_far], rec.at[0], b_s.at[0], b_r.at[0], ahead)
        self.near = send(theirs.at[self.b_near], rec.at[1], b_s.at[1], b_r.at[1], ahead)
        self.back = send(theirs.at[self.b_back], rec.at[2], b_s.at[2], b_r.at[2], behind)
        ahead, behind = at.at(b, a + way), at.at(b, a - way)
        self.far2 = send(theirs.at[b, self.a_far], arec.at[0], a_s.at[0], a_r.at[0], ahead)
        self.near2 = send(theirs.at[b, self.a_near], arec.at[1], a_s.at[1], a_r.at[1], ahead)
        self.back2 = send(theirs.at[b, self.a_back], arec.at[2], a_s.at[2], a_r.at[2], behind)
        self.cross = [send(xs.at[i], xr.at[i], x_s.at[i], x_r.at[i], at.group(i + 1)) for i in range(2)]

    def block(self, b, extra=()):
        @pl.loop(0, SIDE)
        def _(j):
            total = wide(self.mine[b, j]) + wide(self.theirs[b, j])
            for slot in extra:
                total = total + wide(self.rec[slot, j])
            self.theirs[b, j] = total.astype(BF16)

    def line(self, a):
        b = self.at.b
        return wide(self.mine[b, a]) + wide(self.theirs[b, a]) + wide(self.rec[1, a]) + wide(self.rec[2, a])

    def start(self):
        for core in range(2):

            @pl.when(self.at.k == core)
            def _():
                for pair, load in zip(self.pairs[core], self.loads[core]):
                    pair.start()
                    load.start()

    def first(self):
        for pair, load in zip(self.pairs[0], self.loads[0]):
            load.wait()
            pair.wait_recv()
        self.block(self.b_far)
        self.far.start()
        self.block(self.b_back)
        self.back.start()

    def second(self):
        self.far.wait_recv()
        self.block(self.b_near, (0,))
        self.near.start()

    def third(self):
        self.back.wait_recv()
        self.near.wait_recv()
        b = self.at.b
        self.theirs[b, self.a_far] = self.line(self.a_far).astype(BF16)
        self.far2.start()
        self.theirs[b, self.a_back] = self.line(self.a_back).astype(BF16)
        self.back2.start()

    def fourth(self):
        self.far2.wait_recv()
        self.theirs[self.at.b, self.a_near] = (self.line(self.a_near) + wide(self.arec[0])).astype(BF16)
        self.near2.start()

    def fifth(self):
        self.back2.wait_recv()
        self.near2.wait_recv()
        self.xs[0] = (self.line(self.at.a) + wide(self.arec[1]) + wide(self.arec[2])).astype(BF16)
        self.cross[0].start()

    def sixth(self):
        self.cross[0].wait_recv()
        self.xs[1] = (wide(self.xs[0]) + wide(self.xr[0])).astype(BF16)
        self.cross[1].start()

    def last(self):
        self.cross[1].wait_recv()
        self.out[...] = (wide(self.xs[1]) + wide(self.xr[1])).astype(BF16)

    def end(self):
        for copy in self.pairs[0] + [self.far, self.near, self.back, self.far2, self.near2, self.back2] + self.cross:
            copy.wait_send()


class Gather:
    STAGES = ("start", "first", "second", "third", "fourth", "end")

    def __init__(self, at, block, whole, own_s, a_s, a_r, b_s, b_r, p_s, p_r):
        b, a, half = at.b, at.a, block.shape[1] // 2

        def spot(db, da):
            row, column = (b + db) % SIDE, (a + da) % SIDE
            return whole.at[row + at.k * (column - row), column + at.k * (row - column), at.k]

        right, left = at.at(b, a + 1), at.at(b, a - 1)
        up, down = at.at(b + 1, a), at.at(b - 1, a)
        self.own = pltpu.make_async_copy(block, spot(0, 0), own_s)
        self.along = [send(block, spot(0, 0), a_s.at[0], a_r.at[0], right), send(block, spot(0, 0), a_s.at[1], a_r.at[1], left)]
        sides = (pl.ds(0, half), pl.ds(half, half))
        self.along += [
            send(spot(0, da).at[:, side], spot(0, da).at[:, side], a_s.at[2 + i], a_r.at[2 + i], to)
            for i, (da, side, to) in enumerate(((-1, sides[0], right), (1, sides[1], left)))
        ]
        steps = (0, -1, 1, 2)
        self.to_up = [send(block if i == 0 else spot(0, da), spot(0, da), b_s.at[i], b_r.at[i], up) for i, da in enumerate(steps)]
        self.to_down = [send(block if i == 0 else spot(0, da), spot(0, da), b_s.at[4 + i], b_r.at[4 + i], down) for i, da in enumerate(steps)]
        self.far = [
            send(spot(-1 if i < 2 else 1, da), spot(-1 if i < 2 else 1, da), b_s.at[8 + i], b_r.at[8 + i], up if i < 2 else down) for i, da in enumerate(steps)
        ]
        self.pair = [
            send(block if i == 0 and db == 0 else spot(db, da), spot(db, da), p_s.at[4 * j + i], p_r.at[4 * j + i], at.partner())
            for j, db in enumerate((0, -1, 1, 2))
            for i, da in enumerate(steps)
        ]

    def start(self):
        for copy in (self.along[0], self.along[1], self.to_up[0], self.to_down[0], self.pair[0], self.own):
            copy.start()

    def first(self):
        for i in (0, 1):
            self.along[i].wait_recv()
            for copy in (self.along[2 + i], self.to_up[1 + i], self.to_down[1 + i], self.pair[1 + i]):
                copy.start()

    def second(self):
        self.along[2].wait_recv()
        self.along[3].wait_recv()
        for copy in (self.to_up[3], self.to_down[3], self.pair[3]):
            copy.start()

    def third(self):
        for i in range(4):
            for j, arrived in ((4, self.to_up), (8, self.to_down)):
                arrived[i].wait_recv()
                if (i < 2) == (j == 4):
                    self.far[i].start()
                self.pair[j + i].start()

    def fourth(self):
        for i in range(4):
            self.far[i].wait_recv()
            self.pair[12 + i].start()

    def end(self):
        for copy in self.pair:
            copy.wait_recv()
        for copy in self.along + self.to_up + self.to_down + self.far + self.pair:
            copy.wait_send()
        self.own.wait()


DMA = pltpu.SemaphoreType.DMA
GATHER_SCRATCH = 7
SUM_SCRATCH = 15


def gather_scratch():
    return [DMA, DMA((4,)), DMA((4,)), DMA((12,)), DMA((12,)), DMA((16,)), DMA((16,))]


def sum_scratch(rows, columns):
    block = (rows, columns)
    bufs = [pltpu.VMEM((SIDE, SIDE) + block, BF16)] * 2 + [pltpu.VMEM((3, SIDE) + block, BF16), pltpu.VMEM((3,) + block, BF16)]
    bufs += [pltpu.VMEM((2,) + block, BF16)] * 2
    return bufs + [DMA((4,))] * 3 + [DMA((3,))] * 4 + [DMA((2,))] * 2


def neighbours(at, groups):
    near = [at.at(at.b + 1, at.a), at.at(at.b - 1, at.a), at.at(at.b, at.a + 1), at.at(at.b, at.a - 1), at.partner()]
    return near + ([at.group(1), at.group(2)] if groups else [])


def params(collective_id, has_side_effects=True):
    return pltpu.CompilerParams(collective_id=collective_id, has_side_effects=has_side_effects, vmem_limit_bytes=VMEM_BYTES)


def local_params():
    return pltpu.CompilerParams(vmem_limit_bytes=VMEM_BYTES)


def cost(matmuls, mebibytes):
    return pl.CostEstimate(flops=matmuls * 2 * 2048 * 1280 * 4352, bytes_accessed=mebibytes * 2**20, transcendentals=0)


ANY = pl.BlockSpec(memory_space=pl.ANY)
WHOLE = pl.BlockSpec(memory_space=pltpu.VMEM)


def in_turn(tasks):
    for stage in tasks[0].STAGES:
        for task in tasks:
            getattr(task, stage)()


def beside(tasks, steps):
    now = pl.program_id(0)
    for step in sorted(set(sum(map(list, steps), []))):

        @pl.when(now == step)
        def _():
            for stage in range(len(tasks[0].STAGES)):
                for task, when in zip(tasks, steps):
                    if when[stage] == step:
                        getattr(task, task.STAGES[stage])()


def shaped_term(t):
    return t.reshape(SIDE, SIDE, 2, t.shape[0] // 32, t.shape[1])


def whole_shape(block):
    return jax.ShapeDtypeStruct((SIDE, SIDE, 2) + block.shape, BF16)


def flat(whole):
    return whole.reshape(-1, whole.shape[-1])


def gathered(*blocks, collective_id):
    n = len(blocks)

    def kernel(*refs):
        at = Place()
        tasks = [Gather(at, refs[i], refs[n + i], *refs[2 * n + GATHER_SCRATCH * i : 2 * n + GATHER_SCRATCH * (i + 1)]) for i in range(n)]
        meet(neighbours(at, False))
        in_turn(tasks)

    outs = pl.pallas_call(
        kernel,
        out_shape=[whole_shape(b) for b in blocks],
        in_specs=[WHOLE] * n,
        out_specs=[ANY] * n,
        scratch_shapes=gather_scratch() * n,
        compiler_params=params(collective_id),
        cost_estimate=cost(3, 30),
        name="gathered",
    )(*blocks)
    return [flat(o) for o in outs]


def sums_of(at, n, ins, outs, scratch):
    return [Sum(at, 1 if i % 2 == 0 else -1, ins[i], outs[i], *scratch[SUM_SCRATCH * i : SUM_SCRATCH * (i + 1)]) for i in range(n)]


def summed(*terms, collective_id):
    shaped = [shaped_term(t) for t in terms]
    n = len(terms)

    def kernel(*refs):
        at = Place()
        tasks = sums_of(at, n, refs[:n], refs[n : 2 * n], refs[2 * n :])
        meet(neighbours(at, True))
        in_turn(tasks)

    return pl.pallas_call(
        kernel,
        out_shape=[jax.ShapeDtypeStruct(t.shape[3:], BF16) for t in shaped],
        in_specs=[ANY] * n,
        out_specs=[WHOLE] * n,
        scratch_shapes=[one for t in shaped for one in sum_scratch(*t.shape[3:])],
        compiler_params=params(collective_id),
        cost_estimate=cost(4, 60),
        name="summed",
    )(*shaped)


TILE = 256
ROWS = 512


def dot_nt_f32(a, w):
    return lax.dot_general(a, w, (((1,), (1,)), ((), ())), preferred_element_type=F32)


def act_body(g, u):
    return (g * jax.nn.sigmoid(g) * u).astype(BF16)


def act_back(g, u, dm):
    s = jax.nn.sigmoid(g)
    silu = g * s
    return (dm * u * (s + silu * (1.0 - s))).astype(BF16), (dm * silu).astype(BF16)


def whole_block(shape):
    return pl.BlockSpec(shape, lambda j: (0, 0))


def column_block(rows):
    return pl.BlockSpec((rows, TILE), lambda j: (0, j))


def row_block(columns):
    return pl.BlockSpec((TILE, columns), lambda j: (j, 0))


def gate_up(a, gate, up, blocks, collective_id):
    tokens, d = a.shape
    hidden, n = gate.shape[1], len(blocks)
    last = hidden // TILE - 1

    def kernel(a_ref, gate_ref, up_ref, *refs):
        ins, (g_ref, u_ref, m_ref), outs, scratch = refs[:n], refs[n : n + 3], refs[n + 3 : 2 * n + 3], refs[2 * n + 3 :]
        at = Place()
        tasks = [Gather(at, ins[i], outs[i], *scratch[GATHER_SCRATCH * i : GATHER_SCRATCH * (i + 1)]) for i in range(n)]

        @pl.when(pl.program_id(0) == 0)
        def _():
            meet(neighbours(at, False))

        beside(tasks, [GATHER_STEPS] * n)
        for i in range(tokens // ROWS):
            r = pl.ds(i * ROWS, ROWS)
            g, u = dot_f32(a_ref[r], gate_ref[...]), dot_f32(a_ref[r], up_ref[...])
            g_ref[r], u_ref[r], m_ref[r] = g, u, act_body(g, u)

    GATHER_STEPS = (0, 4, 7, 12, 15, last)
    outs = pl.pallas_call(
        kernel,
        grid=(last + 1,),
        out_shape=[jax.ShapeDtypeStruct((tokens, hidden), t) for t in (F32, F32, BF16)] + [whole_shape(b) for b in blocks],
        in_specs=[whole_block((tokens, d)), column_block(d), column_block(d)] + [WHOLE] * n,
        out_specs=[column_block(tokens)] * 3 + [ANY] * n,
        scratch_shapes=gather_scratch() * n,
        compiler_params=params(collective_id),
        cost_estimate=cost(2, 110),
        name="gate_up",
    )(a, gate, up, *blocks)
    return outs[:3], [flat(o) for o in outs[3:]]


def middle(a, dy, gate, up, down):
    tokens, d = a.shape
    hidden = gate.shape[1]

    def kernel(a_ref, dy_ref, gate_ref, up_ref, down_ref, m_ref, dg_ref, du_ref):
        for i in range(tokens // ROWS):
            r = pl.ds(i * ROWS, ROWS)
            g, u = dot_f32(a_ref[r], gate_ref[...]), dot_f32(a_ref[r], up_ref[...])
            dm = wide(dot_nt_f32(dy_ref[r], down_ref[...]).astype(BF16))
            m_ref[r] = act_body(g, u)
            dg_ref[r], du_ref[r] = act_back(g, u, dm)

    return pl.pallas_call(
        kernel,
        grid=(hidden // TILE,),
        out_shape=[jax.ShapeDtypeStruct((tokens, hidden), BF16)] * 3,
        in_specs=[whole_block((tokens, d))] * 2 + [column_block(d)] * 2 + [row_block(d)],
        out_specs=[column_block(tokens)] * 3,
        compiler_params=local_params(),
        cost_estimate=cost(3, 100),
        name="middle",
    )(a, dy, gate, up, down)


def back_down(dy, down, g, u, terms, collective_id):
    tokens, d = dy.shape
    hidden, n = down.shape[0], len(terms)
    shaped = [shaped_term(t) for t in terms]
    last = hidden // TILE - 1
    steps = (0, 4, 8, 13, 15, last, last, last, last)

    def kernel(dy_ref, down_ref, g_ref, u_ref, *refs):
        ins, (dg_ref, du_ref), outs, scratch = refs[:n], refs[n : n + 2], refs[n + 2 : 2 * n + 2], refs[2 * n + 2 :]
        at = Place()
        tasks = sums_of(at, n, ins, outs, scratch)

        @pl.when(pl.program_id(0) == 0)
        def _():
            meet(neighbours(at, True))

        beside(tasks, [steps] * n)
        for i in range(tokens // ROWS):
            r = pl.ds(i * ROWS, ROWS)
            dm = wide(dot_nt_f32(dy_ref[r], down_ref[...]).astype(BF16))
            dg_ref[r], du_ref[r] = act_back(g_ref[r], u_ref[r], dm)

    outs = pl.pallas_call(
        kernel,
        grid=(last + 1,),
        out_shape=[jax.ShapeDtypeStruct((tokens, hidden), BF16)] * 2 + [jax.ShapeDtypeStruct(t.shape[3:], BF16) for t in shaped],
        in_specs=[whole_block((tokens, d)), row_block(d), column_block(tokens), column_block(tokens)] + [ANY] * n,
        out_specs=[column_block(tokens)] * 2 + [WHOLE] * n,
        scratch_shapes=[one for t in shaped for one in sum_scratch(*t.shape[3:])],
        compiler_params=params(collective_id),
        cost_estimate=cost(2, 120),
        name="back_down",
    )(dy, down, g, u, *shaped)
    return outs[:2], outs[2:]


def back_up(dg, du, gate, up, terms, collective_id):
    tokens, hidden = dg.shape
    d, n = gate.shape[0], len(terms)
    shaped = [shaped_term(t) for t in terms]
    last = hidden // TILE - 1
    steps = ((0, 4, 9, 14, last, last, last, last, last), (0, 6, 11, 16, last, last, last, last, last))

    def kernel(dg_ref, du_ref, gate_ref, up_ref, *refs):
        ins, o_ref, outs, (acc, *scratch) = refs[:n], refs[n], refs[n + 1 : 2 * n + 1], refs[2 * n + 1 :]
        at = Place()
        tasks = sums_of(at, n, ins, outs, scratch)
        now = pl.program_id(0)

        @pl.when(now == 0)
        def _():
            meet(neighbours(at, True))

        beside(tasks, steps[:n])
        for i in range(tokens // ROWS):
            r = pl.ds(i * ROWS, ROWS)
            part = dot_nt_f32(dg_ref[r], gate_ref[...]) + dot_nt_f32(du_ref[r], up_ref[...])

            @pl.when(now == 0)
            def _():
                acc[r] = part

            @pl.when(now > 0)
            def _():
                acc[r] += part

        @pl.when(now == last)
        def _():
            o_ref[...] = acc[...].astype(BF16)

    outs = pl.pallas_call(
        kernel,
        grid=(last + 1,),
        out_shape=[jax.ShapeDtypeStruct((tokens, d), BF16)] + [jax.ShapeDtypeStruct(t.shape[3:], BF16) for t in shaped],
        in_specs=[column_block(tokens)] * 2 + [column_block(d)] * 2 + [ANY] * n,
        out_specs=[pl.BlockSpec((tokens, d), lambda j: (0, 0), pipeline_mode=pl.Buffered(1))] + [WHOLE] * n,
        scratch_shapes=[pltpu.VMEM((tokens, d), F32)] + [one for t in shaped for one in sum_scratch(*t.shape[3:])],
        compiler_params=params(collective_id),
        cost_estimate=cost(3, 80),
        name="back_up",
    )(dg, du, gate, up, *shaped)
    return outs[0], outs[1:]


def solution(mesh):
    def fetched(w):
        return lax.all_gather(w, "s", axis=0, tiled=True)

    def scattered(term):
        return lax.psum(lax.psum_scatter(term, "s", scatter_dimension=0, tiled=True), "r")

    def step(x, dy, w_gate, w_up, w_down):
        x, dy = x[0], dy[0]
        down0, down1 = fetched(w_down[0]), fetched(w_down[1])
        gate0, up0 = gathered(w_gate[0], w_up[0], collective_id=1)

        a0, back_norm0 = jax.vjp(normed, x)
        (g0, u0, m0), (gate1, up1) = gate_up(a0, gate0, up0, (w_gate[1], w_up[1]), 2)
        h1 = x + matmul(m0, down0)
        a1, back_norm1 = jax.vjp(normed, h1)
        m1, dg1, du1 = middle(a1, dy, gate1, up1, down1)
        by_down1 = scattered(dot_tn(m1, dy))
        by_gate1 = scattered(dot_tn(a1, dg1))
        by_up1 = scattered(dot_tn(a1, du1))
        by_h1 = dy + back_norm1(dot_nt(dg1, gate1) + dot_nt(du1, up1))[0]

        (dg0, du0), (by_down0,) = back_down(by_h1, down0, g0, u0, (dot_tn(m0, by_h1),), 3)
        by_a0, (by_gate0, by_up0) = back_up(dg0, du0, gate0, up0, (dot_tn(a0, dg0), dot_tn(a0, du0)), 4)
        by_x = by_h1 + back_norm0(by_a0)[0]
        return by_x[None], jnp.stack([by_gate0, by_gate1]), jnp.stack([by_up0, by_up1]), jnp.stack([by_down0, by_down1])

    states, cut = P(("rep", "r", "s"), None, None), P(None, "s", None)
    return jax.shard_map(
        step,
        mesh=mesh,
        in_specs=(states, states) + (cut,) * 3,
        out_specs=(states,) + (P("rep", "s", None),) * 3,
        check_vma=False,
    )
```

```python
import functools

import jax
import jax.numpy as jnp
from jax import lax
from jax.experimental import pallas as pl
from jax.experimental.pallas import tpu as pltpu
from jax.sharding import PartitionSpec as P

F32, BF16 = jnp.float32, jnp.bfloat16
SIDE = 4

VMEM_BYTES = 66 * 2**20 - 2**18


def matmul(a, w):
    return jnp.dot(a, w, preferred_element_type=F32).astype(BF16)


def dot_f32(a, w):
    return jnp.dot(a, w, preferred_element_type=F32)


def dot_nt(a, w):
    return lax.dot_general(a, w, (((1,), (1,)), ((), ())), preferred_element_type=F32).astype(BF16)


def dot_tn(a, w):
    return lax.dot_general(a, w, (((0,), (0,)), ((), ())), preferred_element_type=F32).astype(BF16)


def normed(h):
    wide = h.astype(F32)
    scale = lax.rsqrt(jnp.mean(wide**2, -1, keepdims=True) + 1e-6)
    return (wide * scale).astype(BF16)


def act(gate, up):
    return (jax.nn.silu(gate) * up).astype(BF16)


class Place:
    def __init__(self):
        self.s = lax.axis_index("s")
        self.r = lax.axis_index("r")
        self.k = self.s % 2
        self.y = self.s // (2 * SIDE)
        self.z = (self.s // 2) % SIDE
        self.b = self.y + self.k * (self.z - self.y)
        self.a = self.z + self.k * (self.y - self.z)

    def at(self, b, a):
        b, a = b % SIDE, a % SIDE
        y = b + self.k * (a - b)
        z = a + self.k * (b - a)
        return {"s": (y * SIDE + z) * 2 + self.k}

    def partner(self):
        return {"s": self.s + 1 - 2 * self.k}

    def group(self, bit):
        if bit == 1:
            return {"r": self.r + 1 - 2 * (self.r % 2)}
        return {"r": (self.r + 2) % 4}


MESH = pl.DeviceIdType.MESH


def send(src, dst, send_sem, recv_sem, to):
    return pltpu.make_async_remote_copy(src_ref=src, dst_ref=dst, send_sem=send_sem, recv_sem=recv_sem, device_id=to, device_id_type=MESH)


def meet(devices):
    barrier = pltpu.get_barrier_semaphore()
    for to in devices:
        pl.semaphore_signal(barrier, inc=1, device_id=to, device_id_type=MESH)
    pl.semaphore_wait(barrier, len(devices))


def wide(ref):
    return ref.astype(F32)


class Sum:
    STAGES = ("start", "first", "second", "third", "fourth", "fifth", "sixth", "last", "end")

    def __init__(self, at, way, term, out, mine, theirs, rec, arec, xs, xr, local, pair_s, pair_r, b_s, b_r, a_s, a_r, x_s, x_r):
        self.at, self.out = at, out
        self.mine, self.theirs, self.rec, self.arec, self.xs, self.xr = mine, theirs, rec, arec, xs, xr
        b, a = at.b, at.a
        self.b_far, self.b_near, self.b_back = (b + 2) % SIDE, (b + way) % SIDE, (b - way) % SIDE
        self.a_far, self.a_near, self.a_back = (a + 2) % SIDE, (a + way) % SIDE, (a - way) % SIDE
        self.loads, self.pairs = [[], []], [[], []]
        for j in range(SIDE):
            for core, (own, away) in enumerate(((term.at[j, :, 0], term.at[:, j, 1]), (term.at[:, j, 1], term.at[j, :, 0]))):
                self.loads[core].append(pltpu.make_async_copy(own, mine.at[j], local.at[j]))
                self.pairs[core].append(send(away, theirs.at[j], pair_s.at[j], pair_r.at[j], at.partner()))
        ahead, behind = at.at(b + way, a), at.at(b - way, a)
        self.far = send(theirs.at[self.b_far], rec.at[0], b_s.at[0], b_r.at[0], ahead)
        self.near = send(theirs.at[self.b_near], rec.at[1], b_s.at[1], b_r.at[1], ahead)
        self.back = send(theirs.at[self.b_back], rec.at[2], b_s.at[2], b_r.at[2], behind)
        ahead, behind = at.at(b, a + way), at.at(b, a - way)
        self.far2 = send(theirs.at[b, self.a_far], arec.at[0], a_s.at[0], a_r.at[0], ahead)
        self.near2 = send(theirs.at[b, self.a_near], arec.at[1], a_s.at[1], a_r.at[1], ahead)
        self.back2 = send(theirs.at[b, self.a_back], arec.at[2], a_s.at[2], a_r.at[2], behind)
        self.cross = [send(xs.at[i], xr.at[i], x_s.at[i], x_r.at[i], at.group(i + 1)) for i in range(2)]

    def block(self, b, extra=()):
        @pl.loop(0, SIDE)
        def _(j):
            total = wide(self.mine[b, j]) + wide(self.theirs[b, j])
            for slot in extra:
                total = total + wide(self.rec[slot, j])
            self.theirs[b, j] = total.astype(BF16)

    def line(self, a):
        b = self.at.b
        return wide(self.mine[b, a]) + wide(self.theirs[b, a]) + wide(self.rec[1, a]) + wide(self.rec[2, a])

    def start(self):
        for core in range(2):

            @pl.when(self.at.k == core)
            def _():
                for pair, load in zip(self.pairs[core], self.loads[core]):
                    pair.start()
                    load.start()

    def first(self):
        for pair, load in zip(self.pairs[0], self.loads[0]):
            load.wait()
            pair.wait_recv()
        self.block(self.b_far)
        self.far.start()
        self.block(self.b_back)
        self.back.start()

    def second(self):
        self.far.wait_recv()
        self.block(self.b_near, (0,))
        self.near.start()

    def third(self):
        self.back.wait_recv()
        self.near.wait_recv()
        b = self.at.b
        self.theirs[b, self.a_far] = self.line(self.a_far).astype(BF16)
        self.far2.start()
        self.theirs[b, self.a_back] = self.line(self.a_back).astype(BF16)
        self.back2.start()

    def fourth(self):
        self.far2.wait_recv()
        self.theirs[self.at.b, self.a_near] = (self.line(self.a_near) + wide(self.arec[0])).astype(BF16)
        self.near2.start()

    def fifth(self):
        self.back2.wait_recv()
        self.near2.wait_recv()
        self.xs[0] = (self.line(self.at.a) + wide(self.arec[1]) + wide(self.arec[2])).astype(BF16)
        self.cross[0].start()

    def sixth(self):
        self.cross[0].wait_recv()
        self.xs[1] = (wide(self.xs[0]) + wide(self.xr[0])).astype(BF16)
        self.cross[1].start()

    def last(self):
        self.cross[1].wait_recv()
        self.out[...] = (wide(self.xs[1]) + wide(self.xr[1])).astype(BF16)

    def end(self):
        for copy in self.pairs[0] + [self.far, self.near, self.back, self.far2, self.near2, self.back2] + self.cross:
            copy.wait_send()


class Gather:
    STAGES = ("start", "first", "second", "third", "fourth", "end")

    def __init__(self, at, block, whole, own_s, a_s, a_r, b_s, b_r, p_s, p_r):
        b, a, half = at.b, at.a, block.shape[1] // 2

        def spot(db, da):
            row, column = (b + db) % SIDE, (a + da) % SIDE
            return whole.at[row + at.k * (column - row), column + at.k * (row - column), at.k]

        right, left = at.at(b, a + 1), at.at(b, a - 1)
        up, down = at.at(b + 1, a), at.at(b - 1, a)
        self.own = pltpu.make_async_copy(block, spot(0, 0), own_s)
        self.along = [send(block, spot(0, 0), a_s.at[0], a_r.at[0], right), send(block, spot(0, 0), a_s.at[1], a_r.at[1], left)]
        sides = (pl.ds(0, half), pl.ds(half, half))
        self.along += [
            send(spot(0, da).at[:, side], spot(0, da).at[:, side], a_s.at[2 + i], a_r.at[2 + i], to)
            for i, (da, side, to) in enumerate(((-1, sides[0], right), (1, sides[1], left)))
        ]
        steps = (0, -1, 1, 2)
        self.to_up = [send(block if i == 0 else spot(0, da), spot(0, da), b_s.at[i], b_r.at[i], up) for i, da in enumerate(steps)]
        self.to_down = [send(block if i == 0 else spot(0, da), spot(0, da), b_s.at[4 + i], b_r.at[4 + i], down) for i, da in enumerate(steps)]
        self.far = [
            send(spot(-1 if i < 2 else 1, da), spot(-1 if i < 2 else 1, da), b_s.at[8 + i], b_r.at[8 + i], up if i < 2 else down) for i, da in enumerate(steps)
        ]
        self.pair = [
            send(block if i == 0 and db == 0 else spot(db, da), spot(db, da), p_s.at[4 * j + i], p_r.at[4 * j + i], at.partner())
            for j, db in enumerate((0, -1, 1, 2))
            for i, da in enumerate(steps)
        ]

    def start(self):
        for copy in (self.along[0], self.along[1], self.to_up[0], self.to_down[0], self.pair[0], self.own):
            copy.start()

    def first(self):
        for i in (0, 1):
            self.along[i].wait_recv()
            for copy in (self.along[2 + i], self.to_up[1 + i], self.to_down[1 + i], self.pair[1 + i]):
                copy.start()

    def second(self):
        self.along[2].wait_recv()
        self.along[3].wait_recv()
        for copy in (self.to_up[3], self.to_down[3], self.pair[3]):
            copy.start()

    def third(self):
        for i in range(4):
            for j, arrived in ((4, self.to_up), (8, self.to_down)):
                arrived[i].wait_recv()
                if (i < 2) == (j == 4):
                    self.far[i].start()
                self.pair[j + i].start()

    def fourth(self):
        for i in range(4):
            self.far[i].wait_recv()
            self.pair[12 + i].start()

    def end(self):
        for copy in self.pair:
            copy.wait_recv()
        for copy in self.along + self.to_up + self.to_down + self.far + self.pair:
            copy.wait_send()
        self.own.wait()


DMA = pltpu.SemaphoreType.DMA
GATHER_SCRATCH = 7
SUM_SCRATCH = 15


def gather_scratch():
    return [DMA, DMA((4,)), DMA((4,)), DMA((12,)), DMA((12,)), DMA((16,)), DMA((16,))]


def sum_scratch(rows, columns):
    block = (rows, columns)
    bufs = [pltpu.VMEM((SIDE, SIDE) + block, BF16)] * 2 + [pltpu.VMEM((3, SIDE) + block, BF16), pltpu.VMEM((3,) + block, BF16)]
    bufs += [pltpu.VMEM((2,) + block, BF16)] * 2
    return bufs + [DMA((4,))] * 3 + [DMA((3,))] * 4 + [DMA((2,))] * 2


def neighbours(at, groups):
    near = [at.at(at.b + 1, at.a), at.at(at.b - 1, at.a), at.at(at.b, at.a + 1), at.at(at.b, at.a - 1), at.partner()]
    return near + ([at.group(1), at.group(2)] if groups else [])


def params(collective_id, has_side_effects=True):
    return pltpu.CompilerParams(collective_id=collective_id, has_side_effects=has_side_effects, vmem_limit_bytes=VMEM_BYTES)


def local_params():
    return pltpu.CompilerParams(vmem_limit_bytes=VMEM_BYTES)


def cost(matmuls, mebibytes):
    return pl.CostEstimate(flops=matmuls * 2 * 2048 * 1280 * 4352, bytes_accessed=mebibytes * 2**20, transcendentals=0)


ANY = pl.BlockSpec(memory_space=pl.ANY)
WHOLE = pl.BlockSpec(memory_space=pltpu.VMEM)


def in_turn(tasks):
    for stage in tasks[0].STAGES:
        for task in tasks:
            getattr(task, stage)()


def beside(tasks, steps):
    now = pl.program_id(0)
    for step in sorted(set(sum(map(list, steps), []))):

        @pl.when(now == step)
        def _():
            for stage in range(len(tasks[0].STAGES)):
                for task, when in zip(tasks, steps):
                    if when[stage] == step:
                        getattr(task, task.STAGES[stage])()


def shaped_term(t):
    return t.reshape(SIDE, SIDE, 2, t.shape[0] // 32, t.shape[1])


def whole_shape(block):
    return jax.ShapeDtypeStruct((SIDE, SIDE, 2) + block.shape, BF16)


def flat(whole):
    return whole.reshape(-1, whole.shape[-1])


def gathered(*blocks, collective_id):
    n = len(blocks)

    def kernel(*refs):
        at = Place()
        tasks = [Gather(at, refs[i], refs[n + i], *refs[2 * n + GATHER_SCRATCH * i : 2 * n + GATHER_SCRATCH * (i + 1)]) for i in range(n)]
        meet(neighbours(at, False))
        in_turn(tasks)

    outs = pl.pallas_call(
        kernel,
        out_shape=[whole_shape(b) for b in blocks],
        in_specs=[WHOLE] * n,
        out_specs=[ANY] * n,
        scratch_shapes=gather_scratch() * n,
        compiler_params=params(collective_id),
        cost_estimate=cost(3, 30),
        name="gathered",
    )(*blocks)
    return [flat(o) for o in outs]


def sums_of(at, n, ins, outs, scratch):
    return [Sum(at, 1 if i % 2 == 0 else -1, ins[i], outs[i], *scratch[SUM_SCRATCH * i : SUM_SCRATCH * (i + 1)]) for i in range(n)]


def summed(*terms, collective_id):
    shaped = [shaped_term(t) for t in terms]
    n = len(terms)

    def kernel(*refs):
        at = Place()
        tasks = sums_of(at, n, refs[:n], refs[n : 2 * n], refs[2 * n :])
        meet(neighbours(at, True))
        in_turn(tasks)

    return pl.pallas_call(
        kernel,
        out_shape=[jax.ShapeDtypeStruct(t.shape[3:], BF16) for t in shaped],
        in_specs=[ANY] * n,
        out_specs=[WHOLE] * n,
        scratch_shapes=[one for t in shaped for one in sum_scratch(*t.shape[3:])],
        compiler_params=params(collective_id),
        cost_estimate=cost(4, 60),
        name="summed",
    )(*shaped)


TILE = 256
ROWS = 512


def dot_nt_f32(a, w):
    return lax.dot_general(a, w, (((1,), (1,)), ((), ())), preferred_element_type=F32)


def act_body(g, u):
    return (g * jax.nn.sigmoid(g) * u).astype(BF16)


def act_back(g, u, dm):
    s = jax.nn.sigmoid(g)
    silu = g * s
    return (dm * u * (s + silu * (1.0 - s))).astype(BF16), (dm * silu).astype(BF16)


def whole_block(shape):
    return pl.BlockSpec(shape, lambda j: (0, 0))


def column_block(rows):
    return pl.BlockSpec((rows, TILE), lambda j: (0, j))


def row_block(columns):
    return pl.BlockSpec((TILE, columns), lambda j: (j, 0))


def gate_up(a, gate, up, blocks, collective_id):
    tokens, d = a.shape
    hidden, n = gate.shape[1], len(blocks)
    last = hidden // TILE - 1

    def kernel(a_ref, gate_ref, up_ref, *refs):
        ins, (g_ref, u_ref, m_ref), outs, scratch = refs[:n], refs[n : n + 3], refs[n + 3 : 2 * n + 3], refs[2 * n + 3 :]
        at = Place()
        tasks = [Gather(at, ins[i], outs[i], *scratch[GATHER_SCRATCH * i : GATHER_SCRATCH * (i + 1)]) for i in range(n)]

        @pl.when(pl.program_id(0) == 0)
        def _():
            meet(neighbours(at, False))

        beside(tasks, [GATHER_STEPS] * n)
        for i in range(tokens // ROWS):
            r = pl.ds(i * ROWS, ROWS)
            g, u = dot_f32(a_ref[r], gate_ref[...]), dot_f32(a_ref[r], up_ref[...])
            g_ref[r], u_ref[r], m_ref[r] = g, u, act_body(g, u)

    GATHER_STEPS = (0, 4, 7, 12, 15, last)
    outs = pl.pallas_call(
        kernel,
        grid=(last + 1,),
        out_shape=[jax.ShapeDtypeStruct((tokens, hidden), t) for t in (F32, F32, BF16)] + [whole_shape(b) for b in blocks],
        in_specs=[whole_block((tokens, d)), column_block(d), column_block(d)] + [WHOLE] * n,
        out_specs=[column_block(tokens)] * 3 + [ANY] * n,
        scratch_shapes=gather_scratch() * n,
        compiler_params=params(collective_id),
        cost_estimate=cost(2, 110),
        name="gate_up",
    )(a, gate, up, *blocks)
    return outs[:3], [flat(o) for o in outs[3:]]


def middle(a, dy, gate, up, down):
    tokens, d = a.shape
    hidden = gate.shape[1]

    def kernel(a_ref, dy_ref, gate_ref, up_ref, down_ref, m_ref, dg_ref, du_ref):
        for i in range(tokens // ROWS):
            r = pl.ds(i * ROWS, ROWS)
            g, u = dot_f32(a_ref[r], gate_ref[...]), dot_f32(a_ref[r], up_ref[...])
            dm = wide(dot_nt_f32(dy_ref[r], down_ref[...]).astype(BF16))
            m_ref[r] = act_body(g, u)
            dg_ref[r], du_ref[r] = act_back(g, u, dm)

    return pl.pallas_call(
        kernel,
        grid=(hidden // TILE,),
        out_shape=[jax.ShapeDtypeStruct((tokens, hidden), BF16)] * 3,
        in_specs=[whole_block((tokens, d))] * 2 + [column_block(d)] * 2 + [row_block(d)],
        out_specs=[column_block(tokens)] * 3,
        compiler_params=local_params(),
        cost_estimate=cost(3, 100),
        name="middle",
    )(a, dy, gate, up, down)


def back_down(dy, down, g, u, terms, collective_id):
    tokens, d = dy.shape
    hidden, n = down.shape[0], len(terms)
    shaped = [shaped_term(t) for t in terms]
    last = hidden // TILE - 1
    steps = (0, 4, 8, 13, 15, last, last, last, last)

    def kernel(dy_ref, down_ref, g_ref, u_ref, *refs):
        ins, (dg_ref, du_ref), outs, scratch = refs[:n], refs[n : n + 2], refs[n + 2 : 2 * n + 2], refs[2 * n + 2 :]
        at = Place()
        tasks = sums_of(at, n, ins, outs, scratch)

        @pl.when(pl.program_id(0) == 0)
        def _():
            meet(neighbours(at, True))

        beside(tasks, [steps] * n)
        for i in range(tokens // ROWS):
            r = pl.ds(i * ROWS, ROWS)
            dm = wide(dot_nt_f32(dy_ref[r], down_ref[...]).astype(BF16))
            dg_ref[r], du_ref[r] = act_back(g_ref[r], u_ref[r], dm)

    outs = pl.pallas_call(
        kernel,
        grid=(last + 1,),
        out_shape=[jax.ShapeDtypeStruct((tokens, hidden), BF16)] * 2 + [jax.ShapeDtypeStruct(t.shape[3:], BF16) for t in shaped],
        in_specs=[whole_block((tokens, d)), row_block(d), column_block(tokens), column_block(tokens)] + [ANY] * n,
        out_specs=[column_block(tokens)] * 2 + [WHOLE] * n,
        scratch_shapes=[one for t in shaped for one in sum_scratch(*t.shape[3:])],
        compiler_params=params(collective_id),
        cost_estimate=cost(2, 120),
        name="back_down",
    )(dy, down, g, u, *shaped)
    return outs[:2], outs[2:]


def back_up(dg, du, gate, up, terms, collective_id):
    tokens, hidden = dg.shape
    d, n = gate.shape[0], len(terms)
    shaped = [shaped_term(t) for t in terms]
    last = hidden // TILE - 1
    steps = ((0, 4, 9, 14, last, last, last, last, last), (0, 6, 11, 16, last, last, last, last, last))

    def kernel(dg_ref, du_ref, gate_ref, up_ref, *refs):
        ins, o_ref, outs, (acc, *scratch) = refs[:n], refs[n], refs[n + 1 : 2 * n + 1], refs[2 * n + 1 :]
        at = Place()
        tasks = sums_of(at, n, ins, outs, scratch)
        now = pl.program_id(0)

        @pl.when(now == 0)
        def _():
            meet(neighbours(at, True))

        beside(tasks, steps[:n])
        for i in range(tokens // ROWS):
            r = pl.ds(i * ROWS, ROWS)
            part = dot_nt_f32(dg_ref[r], gate_ref[...]) + dot_nt_f32(du_ref[r], up_ref[...])

            @pl.when(now == 0)
            def _():
                acc[r] = part

            @pl.when(now > 0)
            def _():
                acc[r] += part

        @pl.when(now == last)
        def _():
            o_ref[...] = acc[...].astype(BF16)

    outs = pl.pallas_call(
        kernel,
        grid=(last + 1,),
        out_shape=[jax.ShapeDtypeStruct((tokens, d), BF16)] + [jax.ShapeDtypeStruct(t.shape[3:], BF16) for t in shaped],
        in_specs=[column_block(tokens)] * 2 + [column_block(d)] * 2 + [ANY] * n,
        out_specs=[pl.BlockSpec((tokens, d), lambda j: (0, 0), pipeline_mode=pl.Buffered(1))] + [WHOLE] * n,
        scratch_shapes=[pltpu.VMEM((tokens, d), F32)] + [one for t in shaped for one in sum_scratch(*t.shape[3:])],
        compiler_params=params(collective_id),
        cost_estimate=cost(3, 80),
        name="back_up",
    )(dg, du, gate, up, *shaped)
    return outs[0], outs[1:]


def solution(mesh):
    def fetched(w):
        return lax.all_gather(w, "s", axis=0, tiled=True)

    def scattered(term):
        return lax.psum_scatter(term, "s", scatter_dimension=0, tiled=True)

    def step(x, dy, w_gate, w_up, w_down):
        x, dy = x[0], dy[0]
        down0, down1 = fetched(w_down[0]), fetched(w_down[1])
        gate0, up0 = gathered(w_gate[0], w_up[0], collective_id=1)

        a0, back_norm0 = jax.vjp(normed, x)
        (g0, u0, m0), (gate1, up1) = gate_up(a0, gate0, up0, (w_gate[1], w_up[1]), 2)
        h1 = x + matmul(m0, down0)
        a1, back_norm1 = jax.vjp(normed, h1)
        m1, dg1, du1 = middle(a1, dy, gate1, up1, down1)
        by_down1 = scattered(dot_tn(m1, dy))
        by_gate1 = scattered(dot_tn(a1, dg1))
        by_up1 = scattered(dot_tn(a1, du1))
        by_h1 = dy + back_norm1(dot_nt(dg1, gate1) + dot_nt(du1, up1))[0]

        (dg0, du0), (by_down0,) = back_down(by_h1, down0, g0, u0, (dot_tn(m0, by_h1),), 3)
        t_gate0, t_up0 = dot_tn(a0, dg0), dot_tn(a0, du0)
        t_gate0, t_up0, by_down1, by_gate1, by_up1 = lax.optimization_barrier((t_gate0, t_up0, by_down1, by_gate1, by_up1))
        by_down1, by_gate1, by_up1 = lax.psum((by_down1, by_gate1, by_up1), "r")
        by_a0, (by_gate0, by_up0) = back_up(dg0, du0, gate0, up0, (t_gate0, t_up0), 4)
        by_x = by_h1 + back_norm0(by_a0)[0]
        return by_x[None], jnp.stack([by_gate0, by_gate1]), jnp.stack([by_up0, by_up1]), jnp.stack([by_down0, by_down1])

    states, cut = P(("rep", "r", "s"), None, None), P(None, "s", None)
    return jax.shard_map(
        step,
        mesh=mesh,
        in_specs=(states, states) + (cut,) * 3,
        out_specs=(states,) + (P("rep", "s", None),) * 3,
        check_vma=False,
    )
```
